32 devices in a mesh: mu: 8 (over y, x, core), nu: 4 (over z).
Axes of the slice: x: 2, y: 2, z: 4, core: 2. Of those that a mesh axis runs over, the one named last changes fastest.
Arguments:
- earlier_vectors: float32 [1024, 1024, 512], P('mu', 'nu'), may hold values from -0.72 to 0.72
- pivot_integral_columns: float32 [1024, 1024, 256], P('mu', 'nu'), may hold values from -6 to 6
- diagonal: float32 [1024, 1024], P('mu', 'nu'), may hold values from 2 to 60
- orbitals: float32 [1024, 40], replicated, may hold values from -0.1875 to 0.1875
- pivots: int32 [256], replicated, may hold values from 0 to 1048575, as said below
Outputs:
- transformed: float32 [256, 820], P(('mu', 'nu'))
- updated_diagonal: float32 [1024, 1024], P('mu', 'nu')
The draws below stay inside these ranges and needn't reach their ends.
Inputs may be any that keep to these rules, and one draw needn't show every extreme that they name: The pivots are distinct. The pairs held by one device (a block of 128 first by 256 second AO indices) contain at most 32 pivots, and some block contains exactly 32.
All inputs are finite; a program needn't handle non-finite values.
Results may differ from the reference program's by a relative error of at most 0.0001.
Values sent between devices are 32-bit elements; how exact they have to be, the bound alone decides.
A program may use at most 256 MiB of HBM per device.

```python
import math
import jax
import jax.numpy as jnp
import numpy as np
from jax import lax

NAO = 1024
NVEC = 512
NPIV = 256
NACT = 40
ROWS_MU = 128
COLS_NU = 256
BLOCKS = 32
MOST = 32


def draw_pivots(key, part):
    overall_position_number = BLOCKS * MOST
    hot_count = max(1, NPIV // (4 * MOST))
    key_order, key_score, key_band, key_perm = jax.random.split(jax.random.fold_in(key, 17), 4)
    device_order = jax.random.permutation(key_order, BLOCKS)
    favoured_marker = device_order < hot_count
    position_owner_map = jnp.arange(overall_position_number, dtype=jnp.int32) // MOST
    slot_index = jnp.arange(overall_position_number, dtype=jnp.int32) % MOST
    stochastic_perturbation = jax.random.randint(key_score, (overall_position_number,), 0, 4096)
    preference_increment = jnp.where(favoured_marker[position_owner_map], 8192, 0)
    selection_merit = (stochastic_perturbation + preference_increment) * overall_position_number + jnp.arange(overall_position_number, dtype=jnp.int32)
    top_values, chosen = lax.top_k(selection_merit, NPIV)
    band_size = ROWS_MU * COLS_NU // MOST
    offset = jax.random.randint(key_band, (NPIV,), 0, band_size)
    device = position_owner_map[chosen]
    local_row = slot_index[chosen] * band_size + offset
    grid_nu = NAO // COLS_NU
    row_mu = device // grid_nu * ROWS_MU + local_row // COLS_NU
    col_nu = device % grid_nu * COLS_NU + local_row % COLS_NU
    flat_pair = row_mu * NAO + col_nu
    ordering = jax.random.permutation(key_perm, NPIV)
    return flat_pair[ordering].astype(jnp.int32)


def block_levels(own_key, shape, shards, least, largest):
    def one(position, blocks):
        heights = jax.random.uniform(jax.random.fold_in(jax.random.fold_in(own_key, 6), position), (blocks,), jnp.float32, least / len(shards), largest / len(shards))
        return jnp.repeat(jnp.exp(heights), shape[position] // blocks).reshape((-1,) + (1,) * (len(shape) - position - 1))

    level = one(*shards[0])
    for cut in shards[1:]:
        level = level * one(*cut)
    return level


def normal_values(stream_key, extent, width, most, shards=(), kind=jnp.bfloat16):
    values = jax.random.normal(stream_key, extent, jnp.float32) * width
    if len(shards) > 0:
        values = block_levels(stream_key, extent, shards, -0.22, 0.18) * values
    return jnp.clip(values, min=-most, max=most).astype(kind)


def setup_inputs(seed: int = 0) -> dict:
    arg_keys = jax.random.split(jax.random.key(seed), 6)
    return {
        "earlier_vectors": normal_values(arg_keys[0], (NAO, NAO, NVEC), 0.12, 0.72, ((0, 8), (1, 4)), jnp.float32),
        "pivot_integral_columns": normal_values(arg_keys[1], (NAO, NAO, NPIV), 1.0, 6.0, ((0, 8), (1, 4)), jnp.float32),
        "diagonal": jnp.clip(jnp.exp(math.log(60.0) - 3.4011974 * jax.random.uniform(arg_keys[2], (NAO, NAO), jnp.float32) ** block_levels(arg_keys[2], (NAO, NAO), ((0, 8), (1, 4)), -0.2, 0.2)), 2.0, 60.0),
        "orbitals": normal_values(arg_keys[3], (NAO, NACT), NAO ** -0.5, 0.1875, (), jnp.float32),
        "pivots": draw_pivots(jax.random.fold_in(arg_keys[5], 71), 0),
    }


precise = lax.Precision.HIGHEST

def reference(earlier_vectors, pivot_integral_columns, diagonal, orbitals, pivots):
    row_index, col_index = np.tril_indices(NACT)
    flat_vectors = earlier_vectors.reshape(NAO * NAO, NVEC)
    pivot_rows = jnp.take(flat_vectors, pivots, axis=0)
    pivot_diag = jnp.take(diagonal.reshape(NAO * NAO), pivots)
    residual_diag = pivot_diag - lax.optimization_barrier(jnp.sum(pivot_rows * pivot_rows, axis=1))
    scaling = lax.rsqrt(jnp.maximum(residual_diag, 1.0))
    stride = 32

    def advance(accumulated, start):
        vectors = lax.dynamic_slice_in_dim(earlier_vectors, start, stride, 0).reshape(stride * NAO, NVEC)
        columns = lax.dynamic_slice_in_dim(pivot_integral_columns, start, stride, 0).reshape(stride * NAO, NPIV)
        diag_block = lax.dynamic_slice_in_dim(diagonal, start, stride, 0)
        update = lax.dot_general(vectors, pivot_rows, (((1,), (1,)), ((), ())), precision=precise)
        fresh_vectors = (columns - update) * scaling[None, :]
        new_diag = diag_block - lax.optimization_barrier(jnp.sum(fresh_vectors * fresh_vectors, axis=1)).reshape(stride, NAO)
        orbit_block = lax.dynamic_slice_in_dim(orbitals, start, stride, 0)
        half_done = jnp.einsum('mp,mnj->jpn', orbit_block, fresh_vectors.reshape(stride, NAO, NPIV), precision=precise)
        accumulated = accumulated + jnp.einsum('nq,jpn->jpq', orbitals, half_done, precision=precise)
        return (accumulated, new_diag)
    starts = jnp.arange(NAO // stride, dtype=jnp.int32) * stride
    accumulated, diag_blocks = lax.scan(advance, jnp.zeros((NPIV, NACT, NACT), jnp.float32), starts)
    return (accumulated[:, row_index, col_index], diag_blocks.reshape(NAO, NAO))
```

```python
import functools

import jax
import jax.numpy as jnp
from jax import lax
from jax.experimental import pallas as pl
from jax.experimental.pallas import tpu as pltpu
from jax.sharding import PartitionSpec as P

f32, bf16 = jnp.float32, jnp.bfloat16


def split(x):
    high = x.astype(bf16)
    return high, (x - high.astype(f32)).astype(bf16)


def mm(a, b):
    return jnp.dot(a, b, preferred_element_type=f32)


def block_kernel(rows, pt_ref, pd_ref, om_ref, on_ref, dg_ref, v_ref, b_ref,
                 full_ref, ud_ref, pcat, scale, oncat, half, tri):
    step = pl.program_id(0)
    _, cols, earlier = v_ref.shape
    active = on_ref.shape[0]
    pivots = b_ref.shape[2]

    @pl.when(step == 0)
    def _():
        pt = pt_ref[...]
        high, low = split(pt)
        pcat[0:earlier] = high
        pcat[earlier:2 * earlier] = high
        pcat[2 * earlier:] = low
        residual = pd_ref[...] - jnp.sum(pt * pt, axis=0, keepdims=True)
        scale[...] = lax.rsqrt(jnp.maximum(residual, 1.0))
        ohigh, olow = split(on_ref[...])
        oncat[0:active] = ohigh
        oncat[active:] = olow

    v = v_ref[...].reshape(rows * cols, earlier)
    vh, vl = split(v)
    update = mm(jnp.concatenate([vh, vl, vh], axis=1), pcat[...])
    fresh = (b_ref[...].reshape(rows * cols, pivots) - update) * scale[...]
    orb = oncat[...]
    for r in range(rows):
        f = fresh[r * cols:(r + 1) * cols]
        fh, fl = split(f)
        both = mm(orb, fh)
        t = both[:active] + both[active:] + mm(orb[:active], fl)
        row = step * rows + r
        for k in range(0, pivots, 128):
            half[k // 128, pl.ds(row * active, active), :] = t[:, k:k + 128]
        sq = f * f
        part = sq[:, :128]
        for k in range(128, pivots, 128):
            part = part + sq[:, k:k + 128]
        total = jnp.sum(part.T, axis=0, keepdims=True)
        ud_ref[pl.ds(row, 1), :] = dg_ref[pl.ds(row, 1), :] - total

    @pl.when(step == pl.num_programs(0) - 1)
    def _():
        count = om_ref.shape[1]
        mh, ml = split(om_ref[...])
        mcat = jnp.concatenate([mh, ml], axis=0)
        for q in range(active):
            tq = jnp.concatenate(
                [half[c, pl.ds(q, count, stride=active), :] for c in range(half.shape[0])], axis=1)
            th, tl = split(tq)
            both = mm(mcat, th)
            g = both[:active] + both[active:] + mm(mh, tl)
            for p in range(q, active):
                tri[p * (p + 1) // 2 + q, :] = g[p]
        pairs = full_ref.shape[1]
        full_ref[...] = tri[...].T[:, :pairs]


def local(earlier_vectors, pivot_integral_columns, diagonal, orbitals, pivots):
    rows_mu, cols_nu, earlier = earlier_vectors.shape
    count = pivots.shape[0]
    ao_count, active = orbitals.shape
    size_mu = lax.axis_size("mu")
    size_nu = lax.axis_size("nu")
    index_mu = lax.axis_index("mu")
    index_nu = lax.axis_index("nu")
    pivot_mu = pivots // ao_count
    pivot_nu = pivots % ao_count
    is_owned = (pivot_mu // rows_mu == index_mu) & (pivot_nu // cols_nu == index_nu)
    local_row = pivot_mu % rows_mu * cols_nu + pivot_nu % cols_nu
    picked = jnp.take(earlier_vectors.reshape(rows_mu * cols_nu, earlier), local_row, axis=0)
    picked_diag = jnp.take(diagonal.reshape(rows_mu * cols_nu), local_row)
    joined = jnp.concatenate(
        [picked, jnp.broadcast_to(picked_diag[:, None], (count, 128))], axis=1)
    joined = lax.psum(jnp.where(is_owned[:, None], joined, 0.0), ("mu", "nu"))
    pivot_t = joined[:, :earlier].T
    pivot_diag = joined[:, earlier][None, :]
    orb_mu = lax.dynamic_slice_in_dim(orbitals, index_mu * rows_mu, rows_mu, 0).T
    orb_nu = lax.dynamic_slice_in_dim(orbitals, index_nu * cols_nu, cols_nu, 0).T

    rows = max(1, min(rows_mu, 1024 // cols_nu))
    pairs = active * (active + 1) // 2
    padded = -(-pairs // 128) * 128
    whole = lambda *shape: pl.BlockSpec(shape, lambda i: (0,) * len(shape))
    full, updated = pl.pallas_call(
        functools.partial(block_kernel, rows),
        grid=(rows_mu // rows,),
        out_shape=(jax.ShapeDtypeStruct((count, pairs), f32),
                   jax.ShapeDtypeStruct((rows_mu, cols_nu), f32)),
        in_specs=[
            whole(earlier, count), whole(1, count), whole(active, rows_mu),
            whole(active, cols_nu), whole(rows_mu, cols_nu),
            pl.BlockSpec((rows, cols_nu, earlier), lambda i: (i, 0, 0)),
            pl.BlockSpec((rows, cols_nu, count), lambda i: (i, 0, 0)),
        ],
        out_specs=(whole(count, pairs), whole(rows_mu, cols_nu)),
        scratch_shapes=[
            pltpu.VMEM((3 * earlier, count), bf16),
            pltpu.VMEM((1, count), f32),
            pltpu.VMEM((2 * active, cols_nu), bf16),
            pltpu.VMEM((count // 128, rows_mu * active, 128), f32),
            pltpu.VMEM((padded, count), f32),
        ],
        compiler_params=pltpu.CompilerParams(
            dimension_semantics=("arbitrary",), vmem_limit_bytes=56 * 1024 * 1024),
    )(pivot_t, pivot_diag, orb_mu, orb_nu, diagonal, earlier_vectors, pivot_integral_columns)

    per_device = count // (size_mu * size_nu)
    split_mu = full.reshape(size_mu, size_nu * per_device, pairs)
    summed = lax.psum_scatter(split_mu, "mu", scatter_dimension=0, tiled=True)
    split_nu = summed.reshape(size_nu, per_device, pairs)
    transformed = lax.psum_scatter(split_nu, "nu", scatter_dimension=0, tiled=True)
    return transformed.reshape(per_device, pairs), updated


def solution(mesh):
    placed = (P("mu", "nu", None), P("mu", "nu", None), P("mu", "nu"), P(), P())
    return jax.shard_map(
        local,
        mesh=mesh,
        in_specs=placed,
        out_specs=(P(("mu", "nu"), None), P("mu", "nu")),
        check_vma=False,
    )
```
